8 devices in a mesh: batch: 1 (over z), tp: 2 (over y), sp: 4 (over x, core).
Axes of the slice: x: 2, y: 2, z: 1, core: 2. Of those that a mesh axis runs over, the one named last changes fastest.
Arguments:
- tokens: bfloat16 [8192, 2048], P(('batch', 'sp'))
- glob_pos: int32 [512], P('batch')
- rel_bias: float32 [16, 513], P('tp')
- w_query: bfloat16 [2048, 2048], P(None, 'tp')
- w_key: bfloat16 [2048, 2048], P(None, 'tp')
- w_value: bfloat16 [2048, 2048], P(None, 'tp')
- w_query_glob: bfloat16 [2048, 2048], P(None, 'tp')
- w_out: bfloat16 [2048, 2048], P('tp')
- w_up: bfloat16 [2048, 8192], P(None, 'tp')
- w_down: bfloat16 [8192, 2048], P('tp')
Outputs:
- output: bfloat16 [8192, 2048], P(('batch', 'sp'))
All inputs are finite; a program needn't handle non-finite values.
Results may differ from the reference program's by a relative error of at most 0.0114595.
Values are sent between devices in bfloat16 or wider.
A program may use at most 1 GiB of HBM per device.

```python
import math
import jax
import jax.numpy as jnp
from jax import lax

MODEL_DIM = 2048
NUM_HEADS = 16
HIDDEN_DIM = 8192
WINDOW = 256
NUM_GLOBAL = 512
SEQ_LEN = 8192


def setup_inputs(seed: int = 0, part: int = 0) -> dict:
    part_keys = jax.random.split(jax.random.fold_in(jax.random.key(seed), part), 2)
    shared_keys = jax.random.split(jax.random.key(seed + 1), 9)
    in_scale = MODEL_DIM ** -0.5
    out_scale = ((2 * WINDOW + NUM_GLOBAL) / (3.0 * MODEL_DIM)) ** 0.5
    glob_scale = (math.log(6.0 * SEQ_LEN / (2 * WINDOW + NUM_GLOBAL)) / MODEL_DIM) ** 0.5

    def draw_normal(rand_key, arr_shape, std_dev):
        return (std_dev * jax.random.normal(rand_key, arr_shape, jnp.float32)).astype(jnp.bfloat16)

    square = (MODEL_DIM, MODEL_DIM)
    glob_pos = jnp.sort(jax.random.permutation(part_keys[1], SEQ_LEN)[:NUM_GLOBAL]).astype(jnp.int32)
    return {
        "tokens": draw_normal(part_keys[0], (SEQ_LEN, MODEL_DIM), 1.0),
        "glob_pos": glob_pos,
        "rel_bias": 0.7 * jax.random.normal(shared_keys[0], (NUM_HEADS, 2 * WINDOW + 1), jnp.float32),
        "w_query": draw_normal(shared_keys[1], square, in_scale),
        "w_key": draw_normal(shared_keys[2], square, in_scale),
        "w_value": draw_normal(shared_keys[3], square, in_scale),
        "w_query_glob": draw_normal(shared_keys[4], square, glob_scale),
        "w_out": draw_normal(shared_keys[5], square, out_scale),
        "w_up": draw_normal(shared_keys[6], (MODEL_DIM, HIDDEN_DIM), in_scale),
        "w_down": draw_normal(shared_keys[7], (HIDDEN_DIM, MODEL_DIM), HIDDEN_DIM ** -0.5),
    }


def reference(tokens, glob_pos, rel_bias, w_query, w_key, w_value, w_query_glob, w_out, w_up, w_down):
    head_dim = MODEL_DIM // NUM_HEADS
    score_scale = head_dim ** -0.5
    n_blocks = SEQ_LEN // WINDOW
    heads_shape = (SEQ_LEN, NUM_HEADS, head_dim)

    def project(weight):
        product = jnp.dot(tokens, weight, preferred_element_type=jnp.float32)
        return product.astype(jnp.bfloat16).astype(jnp.float32).reshape(heads_shape)

    queries = project(w_query)
    keys_all = project(w_key)
    values_all = project(w_value)
    zero_pad = jnp.zeros((WINDOW, NUM_HEADS, head_dim), jnp.float32)
    keys_ext = jnp.concatenate([zero_pad, keys_all, zero_pad], axis=0)
    values_ext = jnp.concatenate([zero_pad, values_all, zero_pad], axis=0)
    glob_keys = keys_all[glob_pos]
    glob_values = values_all[glob_pos]
    rel_offs = jnp.arange(3 * WINDOW)[None, :] - jnp.arange(WINDOW)[:, None]
    in_band = (rel_offs >= 0) & (rel_offs <= 2 * WINDOW)
    band_bias = jnp.take(rel_bias, jnp.clip(rel_offs, 0, 2 * WINDOW), axis=1)

    def window_block(blk_index):
        blk_start = blk_index * WINDOW
        q_blk = lax.dynamic_slice_in_dim(queries, blk_start, WINDOW, axis=0)
        k_win = lax.dynamic_slice_in_dim(keys_ext, blk_start, 3 * WINDOW, axis=0)
        v_win = lax.dynamic_slice_in_dim(values_ext, blk_start, 3 * WINDOW, axis=0)
        query_pos = blk_start + jnp.arange(WINDOW)
        key_pos = blk_start - WINDOW + jnp.arange(3 * WINDOW)
        key_ok = (key_pos >= 0) & (key_pos < SEQ_LEN)
        win_scores = jnp.einsum("qhd,khd->hqk", q_blk, k_win) * score_scale + band_bias
        win_scores = jnp.where(in_band & key_ok[None, :], win_scores, -jnp.inf)
        far_mask = jnp.abs(query_pos[:, None] - glob_pos[None, :]) > WINDOW
        glob_scores = jnp.einsum("qhd,ghd->hqg", q_blk, glob_keys) * score_scale
        glob_scores = jnp.where(far_mask, glob_scores, -jnp.inf)
        scores = jnp.concatenate([win_scores, glob_scores], axis=-1)
        attn_probs = jax.nn.softmax(scores, axis=-1).astype(jnp.bfloat16).astype(jnp.float32)
        all_values = jnp.concatenate([v_win, glob_values], axis=0)
        return jnp.einsum("hqk,khd->qhd", attn_probs, all_values)

    win_out = lax.map(window_block, jnp.arange(n_blocks)).reshape(heads_shape)
    x_glob = tokens[glob_pos]
    q_glob = jnp.dot(x_glob, w_query_glob, preferred_element_type=jnp.float32)
    q_glob = q_glob.astype(jnp.bfloat16).astype(jnp.float32).reshape(NUM_GLOBAL // 8, 8, NUM_HEADS, head_dim)

    def glob_block(q_group):
        scores = jnp.einsum("ghd,khd->hgk", q_group, keys_all) * score_scale
        attn_probs = jax.nn.softmax(scores, axis=-1).astype(jnp.bfloat16).astype(jnp.float32)
        return jnp.einsum("hgk,khd->ghd", attn_probs, values_all)

    glob_out = lax.map(glob_block, q_glob).reshape(NUM_GLOBAL, NUM_HEADS, head_dim)
    heads_out = win_out.at[glob_pos].set(glob_out)
    attn_vec = heads_out.reshape(SEQ_LEN, MODEL_DIM).astype(jnp.bfloat16)
    attn_proj = jnp.dot(attn_vec, w_out, preferred_element_type=jnp.float32)
    hidden = (tokens.astype(jnp.float32) + attn_proj).astype(jnp.bfloat16)
    up_proj = jnp.dot(hidden, w_up, preferred_element_type=jnp.float32)
    act_vals = jax.nn.gelu(up_proj).astype(jnp.bfloat16)
    down_proj = jnp.dot(act_vals, w_down, preferred_element_type=jnp.float32)
    return (hidden.astype(jnp.float32) + down_proj).astype(jnp.bfloat16)
```

```python
import functools
import math

import jax
import jax.numpy as jnp
from jax import lax
from jax.experimental import pallas as pl
from jax.experimental.pallas import tpu as pltpu
from jax.sharding import PartitionSpec as P


LOG2E = math.log2(math.e)
LANES = 128
F32 = jnp.float32
BF16 = jnp.bfloat16
NEG = float("-inf")


def dot_nt(lhs, rhs):
    return lax.dot_general(lhs, rhs, (((1,), (1,)), ((), ())), preferred_element_type=F32)


def window_kernel(q_blk, window, seq_len, half_ref, q_ref, k_ref, v_ref, kl_ref, vl_ref, kr_ref, vr_ref,
                  kg_ref, vg_ref, rel_ref, gp_ref, o_ref, k_buf, v_buf, bias, far):
    rows = q_ref.shape[0]
    span = q_blk + 2 * window
    n_blk = rows // q_blk
    local_rows = k_ref.shape[0]
    scale = q_ref.shape[1] ** -0.5 * LOG2E
    row_start = half_ref[1] + half_ref[0] * rows
    sub_start = half_ref[0] * rows

    @pl.when(pl.program_id(0) == 0)
    def _():
        for blk in range(n_blk):
            pos = row_start + blk * q_blk + lax.broadcasted_iota(jnp.int32, (q_blk, far.shape[1]), 0)
            far[pl.ds(blk * q_blk, q_blk), :] = jnp.where(jnp.abs(pos - gp_ref[...]) > window, 0.0, NEG)

    k_buf[pl.ds(0, window), :] = kl_ref[...]
    k_buf[pl.ds(window, local_rows), :] = k_ref[...]
    k_buf[pl.ds(window + local_rows, window), :] = kr_ref[...]
    v_buf[pl.ds(0, window), :] = vl_ref[...]
    v_buf[pl.ds(window, local_rows), :] = v_ref[...]
    v_buf[pl.ds(window + local_rows, window), :] = vr_ref[...]
    base = pltpu.roll(jnp.broadcast_to(rel_ref[0], (q_blk, span)), 0, 1, stride=1, stride_axis=0)
    for blk in range(n_blk):
        key_pos = row_start + blk * q_blk - window + lax.broadcasted_iota(jnp.int32, (1, span), 1)
        ok = (key_pos >= 0) & (key_pos < seq_len)
        edge = blk * q_blk < window or (blk + 1) * q_blk + window > rows
        if edge:
            slot = 1 + (blk if blk * q_blk < window else blk - n_blk + 2 * (window // q_blk))
            bias[slot] = base + jnp.where(ok, 0.0, NEG)
    bias[0] = base

    def step(blk, slot):
        start = blk * q_blk if isinstance(blk, int) else pl.multiple_of(blk * q_blk, q_blk)
        q = q_ref[pl.ds(start, q_blk), :]
        key_start = pl.multiple_of(sub_start + start, LANES)
        win = dot_nt(q, k_buf[pl.ds(key_start, span), :]) * scale + bias[slot]
        glb = dot_nt(q, kg_ref[...]) * scale + far[pl.ds(start, q_blk), :]
        top = jnp.maximum(win.max(axis=-1, keepdims=True), glb.max(axis=-1, keepdims=True))
        win = jnp.exp2(win - top)
        glb = jnp.exp2(glb - top)
        inv = 1.0 / (win.sum(axis=-1, keepdims=True) + glb.sum(axis=-1, keepdims=True))
        out = jnp.dot((win * inv).astype(BF16), v_buf[pl.ds(key_start, span), :], preferred_element_type=F32)
        out = out + jnp.dot((glb * inv).astype(BF16), vg_ref[...], preferred_element_type=F32)
        o_ref[pl.ds(start, q_blk), :] = out.astype(BF16)

    for blk in range(n_blk):
        left = blk * q_blk < window
        right = (blk + 1) * q_blk + window > rows
        step(blk, 1 + blk if left else 1 + blk - n_blk + 2 * (window // q_blk) if right else 0)


def window_attention(info, q, k, v, kl, vl, kr, vr, kg, vg, rel, gp, seq_len, window, q_blk, halves):
    local_rows, width = q.shape
    heads = width // LANES
    rows = local_rows // halves
    span = q_blk + 2 * window
    num_glob = kg.shape[0]

    def whole(n):
        return pl.BlockSpec((n, LANES), lambda h, s: (0, h))

    grid_spec = pltpu.PrefetchScalarGridSpec(
        num_scalar_prefetch=1,
        grid=(heads,),
        in_specs=[
            pl.BlockSpec((rows, LANES), lambda h, s: (s[0], h)),
            whole(local_rows), whole(local_rows),
            whole(window), whole(window), whole(window), whole(window),
            whole(num_glob), whole(num_glob),
            pl.BlockSpec((1, 1, span), lambda h, s: (h, 0, 0)),
            pl.BlockSpec((1, num_glob), lambda h, s: (0, 0)),
        ],
        out_specs=pl.BlockSpec((rows, LANES), lambda h, s: (0, h)),
        scratch_shapes=[
            pltpu.VMEM((local_rows + 2 * window, LANES), BF16),
            pltpu.VMEM((local_rows + 2 * window, LANES), BF16),
            pltpu.VMEM((1 + 2 * (window // q_blk), q_blk, span), F32),
            pltpu.VMEM((rows, num_glob), F32),
        ],
    )
    elems = heads * rows * (span + num_glob)
    return pl.pallas_call(
        functools.partial(window_kernel, q_blk, window, seq_len),
        grid_spec=grid_spec,
        out_shape=jax.ShapeDtypeStruct((rows, width), BF16),
        compiler_params=pltpu.CompilerParams(dimension_semantics=("arbitrary",)),
        cost_estimate=pl.CostEstimate(flops=elems * LANES * 4 * 2, bytes_accessed=4 * 2 * local_rows * width,
                                      transcendentals=elems),
        name="window_attention",
    )(info, q, k, v, kl, vl, kr, vr, kg, vg, rel, gp)


def global_kernel(g_blk, q_ref, k_ref, v_ref, o_ref):
    scale = q_ref.shape[1] ** -0.5 * LOG2E
    head = pl.program_id(0)
    width = o_ref.shape[1] - LANES
    col = pl.ds(pl.multiple_of(head * LANES, LANES), LANES)
    stat = pl.ds(width, LANES)
    for start in range(0, q_ref.shape[0], g_blk):
        rows = pl.ds(start, g_blk)
        s = dot_nt(q_ref[rows, :], k_ref[...]) * scale
        top = s.max(axis=-1, keepdims=True)
        p = jnp.exp2(s - top)
        tot = p.sum(axis=-1, keepdims=True)
        o_ref[rows, col] = jnp.dot(p.astype(BF16), v_ref[...], preferred_element_type=F32)
        lane = lax.broadcasted_iota(jnp.int32, (g_blk, LANES), 1)
        old = jnp.where(head == 0, 0.0, o_ref[rows, stat])
        o_ref[rows, stat] = jnp.where(lane == head, top, jnp.where(lane == head + LANES // 2, tot, old))


def global_partial(q, k, v, g_blk):
    num_glob, width = q.shape
    heads = width // LANES
    rows = k.shape[0]
    elems = heads * rows * num_glob
    col = lambda n: pl.BlockSpec((n, LANES), lambda h: (0, h))
    return pl.pallas_call(
        functools.partial(global_kernel, g_blk),
        grid=(heads,),
        in_specs=[col(num_glob), col(rows), col(rows)],
        out_specs=pl.BlockSpec((num_glob, width + LANES), lambda h: (0, 0)),
        out_shape=jax.ShapeDtypeStruct((num_glob, width + LANES), F32),
        compiler_params=pltpu.CompilerParams(dimension_semantics=("arbitrary",)),
        cost_estimate=pl.CostEstimate(flops=elems * LANES * 4 * 2, bytes_accessed=4 * rows * width,
                                      transcendentals=elems),
        name="global_partial",
    )(q, k, v)


def solution(mesh):
    n_seq = mesh.shape["sp"]
    n_tp = mesh.shape["tp"]
    to_right = [(sender, sender + 1) for sender in range(n_seq - 1)]
    to_left = [(sender + 1, sender) for sender in range(n_seq - 1)]
    swap_tp = [(0, 1), (1, 0)]
    swap_core = [(i, i ^ 1) for i in range(n_seq)]
    swap_x = [(i, i ^ 2) for i in range(n_seq)]

    def local_layer(tokens, glob_pos, rel_bias, w_query, w_key, w_value, w_query_glob, w_out, w_up, w_down):
        local_rows, model = tokens.shape
        local_heads = rel_bias.shape[0]
        window = (rel_bias.shape[1] - 1) // 2
        local_dim = w_query.shape[1]
        num_glob = glob_pos.shape[0]
        seq_len = local_rows * n_seq
        tp = lax.axis_index("tp")
        sp = lax.axis_index("sp")
        core = sp % 2
        xpos = sp // 2
        row_start = sp * local_rows
        rows = local_rows // n_tp
        q_blk = 128

        def tp_swap(value):
            return lax.ppermute(value, "tp", swap_tp)

        def sp_swap(value, perm):
            return lax.ppermute(value, "sp", perm)

        def dot(lhs, rhs):
            return jnp.dot(lhs, rhs, preferred_element_type=F32)

        def project(lhs, rhs):
            return dot(lhs, rhs).astype(BF16)

        def quarter(weight, parts):
            step = weight.shape[0] // n_seq
            width = weight.shape[1] // parts
            return [tp_swap(lax.dynamic_slice(weight, (sp * step, i * width), (step, width)))
                    for i in range(parts)]

        def spread(value):
            return lax.all_gather(value, "sp", axis=0, tiled=True)

        def halves(value, bit):
            half = value.shape[0] // 2
            return (lax.dynamic_slice_in_dim(value, bit * half, half, 0),
                    lax.dynamic_slice_in_dim(value, (1 - bit) * half, half, 0))

        step = w_out.shape[0] // n_seq
        out_q = tp_swap(lax.dynamic_slice_in_dim(w_out, sp * step, step, 0))
        up_q = quarter(w_up, 2)
        down_q = quarter(w_down, 4)

        local_pos = glob_pos - row_start
        pick = (local_pos[:, None] == jnp.arange(local_rows)[None, :]).astype(BF16)
        x_part = project(pick, tokens)
        keep, give = halves(x_part, core)
        keep = keep + sp_swap(give, swap_core)
        keep = keep + sp_swap(keep, swap_x)
        got = sp_swap(keep, swap_core)
        x_glob = jnp.concatenate([jnp.where(core == 0, keep, got), jnp.where(core == 0, got, keep)])

        k_loc = project(tokens, w_key)
        v_loc = project(tokens, w_value)
        kv_l = sp_swap(jnp.stack([k_loc[local_rows - window:], v_loc[local_rows - window:]]), to_right)
        kv_r = sp_swap(jnp.stack([k_loc[:window], v_loc[:window]]), to_left)
        q_loc = project(tokens, w_query)
        qg = project(x_glob, w_query_glob)
        kg = project(x_glob, w_key)
        vg = project(x_glob, w_value)

        state = global_partial(qg, k_loc, v_loc, 128)

        def merge(mine, other):
            top_a, top_b = mine[:, local_dim:local_dim + local_heads], other[:, local_dim:local_dim + local_heads]
            at = local_dim + LANES // 2
            tot_a, tot_b = mine[:, at:at + local_heads], other[:, at:at + local_heads]
            best = jnp.maximum(top_a, top_b)
            fac_a = jnp.exp2(top_a - best)
            fac_b = jnp.exp2(top_b - best)

            def wide(fac):
                return jnp.repeat(fac, LANES, axis=1)

            acc = mine[:, :local_dim] * wide(fac_a) + other[:, :local_dim] * wide(fac_b)
            return acc, best, tot_a * fac_a + tot_b * fac_b

        keep, give = halves(state, core)
        acc, top, tot = merge(keep, sp_swap(give, swap_core))
        fill = jnp.zeros((acc.shape[0], LANES // 2 - local_heads), F32)
        state = jnp.concatenate([acc, top, fill, tot, fill], axis=1)
        keep, give = halves(state, xpos)
        acc, _, tot = merge(keep, sp_swap(give, swap_x))
        g_mine = (acc / jnp.repeat(tot, LANES, axis=1)).astype(BF16)
        g_pair = jnp.concatenate([g_mine, tp_swap(g_mine)], axis=1)
        g_half = jnp.concatenate([g_pair, sp_swap(g_pair, swap_x)])
        g_all = jnp.concatenate([g_half, sp_swap(g_half, swap_core)])
        part = num_glob // n_seq
        order = [core * 2 + xpos, core * 2 + 1 - xpos, (1 - core) * 2 + xpos, (1 - core) * 2 + 1 - xpos]
        gp_order = jnp.concatenate([lax.dynamic_slice_in_dim(glob_pos, i * part, part) for i in order])

        span = q_blk + 2 * window
        rel = jnp.concatenate([rel_bias * LOG2E, jnp.full((local_heads, span - rel_bias.shape[1]), NEG, F32)], axis=1)
        rel = rel[:, None, :]
        gp = glob_pos[None, :]

        def attend(unit, parts):
            info = jnp.stack([unit, row_start]).astype(jnp.int32)
            return window_attention(info, q_loc, k_loc, v_loc, kv_l[0], kv_l[1], kv_r[0], kv_r[1], kg, vg, rel, gp,
                                    seq_len, window, q_blk, parts)

        o_give = attend(1 - tp, n_tp)
        o_other = tp_swap(o_give)
        o_own = jnp.concatenate([attend(2 * tp, 2 * n_tp), attend(2 * tp + 1, 2 * n_tp)])

        my_pos = row_start + tp * rows + jnp.arange(rows)
        place = my_pos[:, None] == gp_order[None, :]
        is_glob = place.any(axis=1)[:, None]
        place = place.astype(BF16)
        o_own = jnp.where(is_glob, dot(place, g_all[:, :local_dim]).astype(BF16), o_own)
        o_other = jnp.where(is_glob, dot(place, g_all[:, local_dim:]).astype(BF16), o_other)

        x_mine = lax.dynamic_slice_in_dim(tokens, tp * rows, rows, 0)
        proj = dot(o_own, w_out)
        hidden = (x_mine.astype(F32) + (proj + dot(o_other, spread(out_q)))).astype(BF16)
        acts = [jax.nn.gelu(dot(hidden, w_up)).astype(BF16)]
        for piece in up_q:
            acts.append(jax.nn.gelu(dot(hidden, spread(piece))).astype(BF16))
        width = acts[1].shape[1]
        cols = model // len(down_q)
        out = jnp.zeros((local_rows, model), BF16)
        for i, piece in enumerate(down_q):
            sl = slice(i * cols, (i + 1) * cols)
            w_piece = spread(piece)
            total = dot(acts[0], w_down[:, sl])
            for j in range(len(up_q)):
                total = total + dot(acts[1 + j], w_piece[j * width:(j + 1) * width])
            mine = (hidden[:, sl].astype(F32) + total).astype(BF16)
            out = lax.dynamic_update_slice(out, mine, (tp * rows, i * cols))
            out = lax.dynamic_update_slice(out, tp_swap(mine), ((1 - tp) * rows, i * cols))
        return out

    row_spec = P(("batch", "sp"), None)
    col_spec = P(None, "tp")
    head_spec = P("tp", None)
    in_specs = (row_spec, P("batch"), head_spec, col_spec, col_spec, col_spec, col_spec, head_spec, col_spec, head_spec)
    return jax.shard_map(local_layer, mesh=mesh, in_specs=in_specs, out_specs=row_spec, check_vma=False)
```

```python
import functools
import math

import jax
import jax.numpy as jnp
from jax import lax
from jax.experimental import pallas as pl
from jax.experimental.pallas import tpu as pltpu
from jax.sharding import PartitionSpec as P


LOG2E = math.log2(math.e)
LANES = 128
F32 = jnp.float32
BF16 = jnp.bfloat16
NEG = float("-inf")


def dot_nt(lhs, rhs):
    return lax.dot_general(lhs, rhs, (((1,), (1,)), ((), ())), preferred_element_type=F32)


def window_kernel(window, seq_len, info, q_ref, k_ref, v_ref, kl_ref, vl_ref, kr_ref, vr_ref,
                  kg_ref, vg_ref, rel_ref, gp_ref, o_ref, k_buf, v_buf, bias, far):
    rows = q_ref.shape[0]
    q_blk = window
    span = q_blk + 2 * window
    n_blk = rows // q_blk
    inner = rows + window
    scale = q_ref.shape[1] ** -0.5 * LOG2E
    row_start = info[1] + info[0] * rows

    @pl.when(pl.program_id(0) == 0)
    def _():
        for blk in range(n_blk):
            pos = row_start + blk * q_blk + lax.broadcasted_iota(jnp.int32, (q_blk, far.shape[1]), 0)
            far[pl.ds(blk * q_blk, q_blk), :] = jnp.where(jnp.abs(pos - gp_ref[...]) > window, 0.0, NEG)

    @pl.when(info[0] == 0)
    def _():
        for buf, ref, halo in ((k_buf, k_ref, kl_ref), (v_buf, v_ref, vl_ref)):
            buf[pl.ds(0, window), :] = halo[...]
            buf[pl.ds(window, inner), :] = ref[pl.ds(0, inner), :]

    @pl.when(info[0] == 1)
    def _():
        for buf, ref, halo in ((k_buf, k_ref, kr_ref), (v_buf, v_ref, vr_ref)):
            buf[pl.ds(0, inner), :] = ref[pl.ds(k_ref.shape[0] - inner, inner), :]
            buf[pl.ds(inner, window), :] = halo[...]

    base = pltpu.roll(jnp.broadcast_to(rel_ref[0], (q_blk, span)), 0, 1, stride=1, stride_axis=0)
    bias[0] = base
    for slot, blk in ((1, 0), (2, n_blk - 1)):
        key_pos = row_start + (blk - 1) * q_blk + lax.broadcasted_iota(jnp.int32, (1, span), 1)
        bias[slot] = base + jnp.where((key_pos >= 0) & (key_pos < seq_len), 0.0, NEG)

    for blk in range(n_blk):
        mine = pl.ds(blk * q_blk, q_blk)
        keys = pl.ds(blk * q_blk, span)
        slot = 1 if blk == 0 else 2 if blk == n_blk - 1 else 0
        q = q_ref[mine, :]
        win = dot_nt(q, k_buf[keys, :]) * scale + bias[slot]
        glb = dot_nt(q, kg_ref[...]) * scale + far[mine, :]
        top = jnp.maximum(win.max(axis=-1, keepdims=True), glb.max(axis=-1, keepdims=True))
        win = jnp.exp2(win - top)
        glb = jnp.exp2(glb - top)
        inv = 1.0 / (win.sum(axis=-1, keepdims=True) + glb.sum(axis=-1, keepdims=True))
        out = jnp.dot((win * inv).astype(BF16), v_buf[keys, :], preferred_element_type=F32)
        out = out + jnp.dot((glb * inv).astype(BF16), vg_ref[...], preferred_element_type=F32)
        o_ref[mine, :] = out.astype(BF16)


def window_attention(info, q, k, v, kv_l, kv_r, kg, vg, rel, gp, seq_len, window):
    local_rows, width = k.shape
    rows = local_rows // 2
    heads = width // LANES
    span = 3 * window
    num_glob = kg.shape[0]

    def whole(n, blk=0):
        return pl.BlockSpec((n, LANES), lambda h, s: (blk, h))

    grid_spec = pltpu.PrefetchScalarGridSpec(
        num_scalar_prefetch=1,
        grid=(heads,),
        in_specs=[
            pl.BlockSpec((rows, LANES), lambda h, s: (s[0], h)), whole(local_rows), whole(local_rows),
            whole(window), whole(window, 1), whole(window), whole(window, 1),
            whole(num_glob), whole(num_glob),
            pl.BlockSpec((1, 1, span), lambda h, s: (h, 0, 0)),
            pl.BlockSpec((1, num_glob), lambda h, s: (0, 0)),
        ],
        out_specs=whole(rows),
        scratch_shapes=[
            pltpu.VMEM((rows + 2 * window, LANES), BF16),
            pltpu.VMEM((rows + 2 * window, LANES), BF16),
            pltpu.VMEM((3, window, span), F32),
            pltpu.VMEM((rows, num_glob), F32),
        ],
    )
    elems = heads * rows * (span + num_glob)
    return pl.pallas_call(
        functools.partial(window_kernel, window, seq_len),
        grid_spec=grid_spec,
        out_shape=jax.ShapeDtypeStruct((rows, width), BF16),
        compiler_params=pltpu.CompilerParams(dimension_semantics=("arbitrary",)),
        cost_estimate=pl.CostEstimate(flops=elems * LANES * 4 * 2, bytes_accessed=4 * 2 * local_rows * width,
                                      transcendentals=elems),
        name="window",
    )(info, q, k, v, kv_l, kv_l, kv_r, kv_r, kg, vg, rel, gp)


def cut_kernel(info, *refs):
    half = len(refs) // 2
    for source, target in zip(refs[:half], refs[half:]):
        target[...] = source[...]


def cut(info, items, n_cut):
    steps = 4
    ins, outs, shapes = [], [], []
    for weight, cols, col in items:
        rows = weight.shape[0] // n_cut
        ins.append(pl.BlockSpec((rows // steps, cols), lambda i, s, col=col: (s[0] * steps + i, col)))
        outs.append(pl.BlockSpec((rows // steps, cols), lambda i, s: (i, 0)))
        shapes.append(jax.ShapeDtypeStruct((rows, cols), BF16))
    return pl.pallas_call(
        cut_kernel,
        grid_spec=pltpu.PrefetchScalarGridSpec(num_scalar_prefetch=1, grid=(steps,), in_specs=ins, out_specs=outs),
        out_shape=shapes,
        compiler_params=pltpu.CompilerParams(dimension_semantics=("arbitrary",)),
        cost_estimate=pl.CostEstimate(flops=10**9, bytes_accessed=10**7, transcendentals=0),
    )(info, *[weight for weight, _, _ in items])


def project_kernel(x_ref, w_ref, o_ref):
    o_ref[...] = jnp.dot(x_ref[...], w_ref[...], preferred_element_type=F32).astype(BF16)


def project_rows(tokens, weight):
    rows, model = tokens.shape
    width = weight.shape[1]
    step = 512
    return pl.pallas_call(
        project_kernel,
        grid=(rows // step,),
        in_specs=[pl.BlockSpec((step, model), lambda i: (i, 0)), fixed(weight.shape)],
        out_specs=pl.BlockSpec((step, width), lambda i: (i, 0)),
        out_shape=jax.ShapeDtypeStruct((rows, width), BF16),
        compiler_params=pltpu.CompilerParams(dimension_semantics=("arbitrary",)),
        cost_estimate=pl.CostEstimate(flops=2 * rows * width * model, bytes_accessed=4 * width * model, transcendentals=0),
        name="project",
    )(tokens, weight)


def global_kernel(g_blk, q_ref, k_ref, v_ref, o_ref):
    scale = q_ref.shape[1] ** -0.5 * LOG2E
    head = pl.program_id(0)
    width = o_ref.shape[1] - LANES
    col = pl.ds(pl.multiple_of(head * LANES, LANES), LANES)
    stat = pl.ds(width, LANES)
    for start in range(0, q_ref.shape[0], g_blk):
        rows = pl.ds(start, g_blk)
        s = dot_nt(q_ref[rows, :], k_ref[...]) * scale
        top = s.max(axis=-1, keepdims=True)
        p = jnp.exp2(s - top)
        tot = p.sum(axis=-1, keepdims=True)
        o_ref[rows, col] = jnp.dot(p.astype(BF16), v_ref[...], preferred_element_type=F32)
        lane = lax.broadcasted_iota(jnp.int32, (g_blk, LANES), 1)
        old = jnp.where(head == 0, 0.0, o_ref[rows, stat])
        o_ref[rows, stat] = jnp.where(lane == head, top, jnp.where(lane == head + LANES // 2, tot, old))


def global_partial(q, k, v, g_blk):
    num_glob, width = q.shape
    heads = width // LANES
    rows = k.shape[0]
    elems = heads * rows * num_glob
    col = lambda n: pl.BlockSpec((n, LANES), lambda h: (0, h))
    return pl.pallas_call(
        functools.partial(global_kernel, g_blk),
        grid=(heads,),
        in_specs=[col(num_glob), col(rows), col(rows)],
        out_specs=pl.BlockSpec((num_glob, width + LANES), lambda h: (0, 0)),
        out_shape=jax.ShapeDtypeStruct((num_glob, width + LANES), F32),
        compiler_params=pltpu.CompilerParams(dimension_semantics=("arbitrary",)),
        cost_estimate=pl.CostEstimate(flops=elems * LANES * 4 * 2, bytes_accessed=4 * rows * width,
                                      transcendentals=elems),
        name="partial",
    )(q, k, v)


def quarters(me):
    core = me + 1 - 2 * lax.rem(me, 2)
    return me, lax.rem(me + 2, 4), core, lax.rem(core + 2, 4)


def aligned(index, size):
    return pl.ds(pl.multiple_of(index * size, size), size)


def fixed(shape, index=(0, 0)):
    return pl.BlockSpec(shape, lambda *_: index, pipeline_mode=pl.Buffered(1))


def out_kernel(info, x_ref, own_ref, oth_ref, g_ref, gp_ref, w_ref, m_ref, mx_ref, mc_ref, md_ref, h_ref, w_oth):
    i = pl.program_id(0)
    step, _ = x_ref.shape
    heads = w_ref.shape[0]
    part = m_ref.shape[0]

    @pl.when(i == 0)
    def _():
        for q, ref in zip(quarters(info[0]), (m_ref, mx_ref, mc_ref, md_ref)):
            w_oth[aligned(q, part), :] = ref[...]

    pos = info[1] + i * step + lax.broadcasted_iota(jnp.int32, (step, gp_ref.shape[1]), 0)
    hit = jnp.where(pos == gp_ref[...], 1.0, 0.0)
    is_glob = hit.max(axis=-1, keepdims=True) > 0.5
    hit = hit.astype(BF16)
    fix = jnp.dot(hit, g_ref[...], preferred_element_type=F32)
    own = jnp.where(is_glob, fix[:, :heads], own_ref[...].astype(F32)).astype(BF16)
    oth = jnp.where(is_glob, fix[:, heads:], oth_ref[...].astype(F32)).astype(BF16)
    total = jnp.dot(own, w_ref[...], preferred_element_type=F32) + jnp.dot(oth, w_oth[...], preferred_element_type=F32)
    h_ref[...] = (x_ref[...].astype(F32) + total).astype(BF16)


def out_proj(info, tokens, own, oth, g_all, gp_order, w_out, bufs, part):
    model = tokens.shape[1]
    heads = w_out.shape[0]
    rows = own.shape[0]
    step = 256
    n = rows // step
    grid_spec = pltpu.PrefetchScalarGridSpec(
        num_scalar_prefetch=1,
        grid=(n,),
        in_specs=[
            pl.BlockSpec((step, model), lambda i, s: (s[2] * n + i, 0)),
            pl.BlockSpec((step, heads), lambda i, s: (i, 0)),
            pl.BlockSpec((step, heads), lambda i, s: (i, 0)),
            fixed(g_all.shape), fixed(gp_order.shape), fixed(w_out.shape),
        ] + [fixed((part, model))] * 4,
        out_specs=pl.BlockSpec((step, model), lambda i, s: (i, 0)),
        scratch_shapes=[pltpu.VMEM((heads, model), BF16)],
    )
    return pl.pallas_call(
        out_kernel,
        grid_spec=grid_spec,
        out_shape=jax.ShapeDtypeStruct((rows, model), BF16),
        compiler_params=pltpu.CompilerParams(dimension_semantics=("arbitrary",)),
        cost_estimate=pl.CostEstimate(flops=4 * rows * heads * model, bytes_accessed=8 * heads * model, transcendentals=0),
        name="out_proj",
    )(info, tokens, own, oth, g_all, gp_order, w_out, *bufs)


def up_kernel(n_own, n_a, info, h_ref, w_ref, *refs):
    a_refs, b_refs, (o_ref, w_cat) = refs[:4], refs[4:8], refs[8:]
    part = a_refs[0].shape[0]
    i = pl.program_id(0)

    def multiply(w):
        o_ref[...] = jax.nn.gelu(jnp.dot(h_ref[...], w[...], preferred_element_type=F32)).astype(BF16)

    def fill(group):
        for q, ref in zip(quarters(info[0]), group):
            w_cat[aligned(q, part), :] = ref[...]

    pl.when(i < n_own)(lambda: multiply(w_ref))
    pl.when((i >= n_own) & (i < n_own + n_a))(lambda: fill(a_refs))
    pl.when(i >= n_own + n_a)(lambda: fill(b_refs))
    pl.when(i >= n_own)(lambda: multiply(w_cat))


def up_proj(info, hidden, w_up, bufs_a, bufs_b, part):
    rows, model = hidden.shape
    units = w_up.shape[1]
    tile = 512
    n_own = units // tile
    n_a = n_own // 2
    spec_a = pl.BlockSpec((part, tile), lambda i, s: (0, jnp.clip(i - n_own, 0, n_a - 1)))
    spec_b = pl.BlockSpec((part, tile), lambda i, s: (0, jnp.maximum(i - n_own - n_a, 0)))
    grid_spec = pltpu.PrefetchScalarGridSpec(
        num_scalar_prefetch=1,
        grid=(2 * n_own,),
        in_specs=[fixed(hidden.shape), pl.BlockSpec((model, tile), lambda i, s: (0, jnp.minimum(i, n_own - 1)))]
        + [spec_a] * 4 + [spec_b] * 4,
        out_specs=pl.BlockSpec((rows, tile), lambda i, s: (0, i)),
        scratch_shapes=[pltpu.VMEM((model, tile), BF16)],
    )
    return pl.pallas_call(
        functools.partial(up_kernel, n_own, n_a),
        grid_spec=grid_spec,
        out_shape=jax.ShapeDtypeStruct((rows, 2 * units), BF16),
        compiler_params=pltpu.CompilerParams(dimension_semantics=("arbitrary",)),
        cost_estimate=pl.CostEstimate(flops=4 * rows * units * model, bytes_accessed=4 * units * model,
                                      transcendentals=2 * rows * units),
        name="up",
    )(info, hidden, w_up, *bufs_a, *bufs_b)


def down_kernel(n_piece, present, hid_ref, act_ref, w_ref, *refs):
    n_buf = 4 * n_piece
    n_here = sum(present)
    n_land = 4 * len(present) - n_here
    bufs, here = refs[:n_buf], list(refs[n_buf:n_buf + n_here])
    out_ref, act, w_cat, stage, *landing = refs[n_buf + n_here:n_buf + n_here + 4 + n_land]
    hop_send, hop_recv, act_sem, local_sem, send_sem, recv_sem = refs[n_buf + n_here + 4 + n_land:]
    n = pl.program_id(0)
    n_tiles = pl.num_programs(0)
    rows, tile = hid_ref.shape
    units = w_ref.shape[0]
    per = here[0].shape[1] // tile
    unit = here[0].shape[0]
    step = 256
    n_part = rows // step
    tp = lax.axis_index("tp")
    me = lax.axis_index("sp")
    _, over_x, over_core, _ = quarters(me)

    def remote(src, dst, send, recv, device):
        return pltpu.make_async_remote_copy(src_ref=src, dst_ref=dst, send_sem=send, recv_sem=recv, device_id=device,
                                            device_id_type=pl.DeviceIdType.MESH)

    def load(r):
        return pltpu.make_async_copy(act_ref.at[aligned(r, step), :], act.at[aligned(r, step), :], act_sem.at[r])

    hops, groups, count = [], [], 0
    for n_present in present:
        group = [here.pop(0) for _ in range(n_present)]
        group += [landing.pop(0) for _ in range(4 - n_present)]
        ways = ((group[0], group[1], over_x), (group[0], group[2], over_core), (group[1], group[3], over_core))
        hop = []
        for source, target, device in ways[n_present - 1:]:
            hop.append(remote(source, target, hop_send.at[count], hop_recv.at[count], {"sp": device}))
            count += 1
        hops.append(hop)
        groups.append(group)

    @pl.when(n == 0)
    def _():
        for r in range(n_part):
            load(r).start()
        barrier = pltpu.get_barrier_semaphore()
        for device in ({"tp": 1 - tp}, {"sp": over_x}, {"sp": over_core}):
            pl.semaphore_signal(barrier, inc=1, device_id=device, device_id_type=pl.DeviceIdType.MESH)
        pl.semaphore_wait(barrier, 3)
        for hop in hops:
            for copy in hop[:2]:
                copy.start()

    for i, hop in enumerate(hops):
        @pl.when(n == per * (n_piece + i))
        def _(hop=hop):
            hop[0].wait_recv()
            if len(hop) == 3:
                hop[2].start()
            for copy in hop[1:]:
                copy.wait_recv()

    def fill(group, cols):
        for q, ref in zip(quarters(me), group):
            def body(r, carry, q=q, ref=ref):
                w_cat[pl.ds(pl.multiple_of(q * unit + r * step, step), step), :] = ref[aligned(r, step), cols]
                return carry

            lax.fori_loop(0, unit // step, body, 0)

    for p in range(n_piece):
        pl.when(n // per == p)(lambda p=p: fill(bufs[4 * p:4 * p + 4], slice(None)))
    for i, group in enumerate(groups):
        for t in range(per):
            pl.when(n == per * (n_piece + i) + t)(
                lambda group=group, t=t: fill(group, slice(t * tile, (t + 1) * tile)))

    def copies(index, r):
        there = out_ref.at[pl.ds(pl.multiple_of(tp * rows + r * step, step), step), aligned(index, tile)]
        here = stage.at[index, aligned(r, step), :]
        return (pltpu.make_async_copy(here, there, local_sem.at[index, r]),
                remote(here, there, send_sem.at[index, r], recv_sem.at[index, r], {"tp": 1 - tp}))

    def compute(r, carry):
        part = aligned(r, step)

        @pl.when(n == 0)
        def _():
            load(r).wait()

        total = jnp.dot(act[part, :units], w_ref[...], preferred_element_type=F32)
        total = total + jnp.dot(act[part, units:], w_cat[...], preferred_element_type=F32)
        stage[n, part, :] = (hid_ref[part, :].astype(F32) + total).astype(BF16)
        near, away = copies(n, r)
        away.start()
        near.start()
        return carry

    lax.fori_loop(0, n_part, compute, 0)

    @pl.when(n == n_tiles - 1)
    def _():
        def drain(index, carry):
            for r in range(n_part):
                near, away = copies(index, r)
                near.wait()
                away.wait()
            return carry

        lax.fori_loop(0, n_tiles, drain, 0)
        for hop in hops:
            for copy in hop:
                copy.wait_send()


def down_proj(hidden, act, w_down, pieces, lasts, out_rows):
    rows, model = hidden.shape
    units = w_down.shape[0]
    unit, width = lasts[0][0].shape
    present = tuple(len(group) for group in lasts)
    n_land = 4 * len(lasts) - sum(present)
    here = [buf for group in lasts for buf in group]
    tile = 256
    per = width // tile
    n = model // tile
    n_part = rows // 256
    specs, bufs = [], []
    for p, group in enumerate(pieces):
        specs += [pl.BlockSpec((unit, tile), lambda i, p=p: (0, jnp.clip(i - per * p, 0, per - 1)))] * 4
        bufs += list(group)
    dma = pltpu.SemaphoreType.DMA
    return pl.pallas_call(
        functools.partial(down_kernel, len(pieces), present),
        grid=(n,),
        in_specs=[pl.BlockSpec((rows, tile), lambda i: (0, i)), pl.BlockSpec(memory_space=pl.ANY),
                  pl.BlockSpec((units, tile), lambda i: (0, i))] + specs + [fixed((unit, width))] * len(here),
        out_specs=pl.BlockSpec(memory_space=pl.ANY),
        out_shape=jax.ShapeDtypeStruct((out_rows, model), BF16),
        scratch_shapes=[
            pltpu.VMEM(act.shape, BF16),
            pltpu.VMEM((units, tile), BF16),
            pltpu.VMEM((n, rows, tile), BF16),
        ] + [pltpu.VMEM((unit, width), BF16)] * n_land + [
            dma((n_land,)), dma((n_land,)), dma((n_part,)), dma((n, n_part)), dma((n, n_part)),
            dma((n, n_part)),
        ],
        compiler_params=pltpu.CompilerParams(dimension_semantics=("arbitrary",), collective_id=0, has_side_effects=True,
                                             vmem_limit_bytes=60 * 2**20),
        cost_estimate=pl.CostEstimate(flops=4 * rows * units * model, bytes_accessed=8 * units * model, transcendentals=0),
        name="down",
    )(hidden, act, w_down, *bufs, *here)


def solution(mesh):
    n_seq = mesh.shape["sp"]
    n_tp = mesh.shape["tp"]
    to_right = [(sender, sender + 1) for sender in range(n_seq - 1)]
    to_left = [(sender + 1, sender) for sender in range(n_seq - 1)]
    swap_tp = [(0, 1), (1, 0)]
    swap_core = [(i, i ^ 1) for i in range(n_seq)]
    swap_x = [(i, i ^ 2) for i in range(n_seq)]

    def local_layer(tokens, glob_pos, rel_bias, w_query, w_key, w_value, w_query_glob, w_out, w_up, w_down):
        local_rows, model = tokens.shape
        local_heads = rel_bias.shape[0]
        window = (rel_bias.shape[1] - 1) // 2
        local_dim = w_query.shape[1]
        num_glob = glob_pos.shape[0]
        seq_len = local_rows * n_seq
        tp = lax.axis_index("tp")
        sp = lax.axis_index("sp")
        core = sp % 2
        xpos = sp // 2
        row_start = sp * local_rows
        rows = local_rows // n_tp

        def tp_swap(value):
            return lax.ppermute(value, "tp", swap_tp)

        def sp_swap(value, perm):
            return lax.ppermute(value, "sp", perm)

        def dot(lhs, rhs):
            return jnp.dot(lhs, rhs, preferred_element_type=F32)

        def project(lhs, rhs):
            return dot(lhs, rhs).astype(BF16)

        def hop(piece):
            mine = tp_swap(piece)
            there = sp_swap(mine, swap_x)
            return mine, there, sp_swap(mine, swap_core), sp_swap(there, swap_core)

        def halves(value, bit):
            half = value.shape[0] // 2
            return (lax.dynamic_slice_in_dim(value, bit * half, half, 0),
                    lax.dynamic_slice_in_dim(value, (1 - bit) * half, half, 0))

        part_out, part_up = local_dim // n_seq, model // n_seq
        cols = model // 4
        me = sp[None].astype(jnp.int32)
        piece_o, piece_a = cut(me, ((w_out, model, 0), (w_up, model, 0)), n_seq)
        piece_b, *piece_down = cut(me, ((w_up, model, 1),) + tuple((w_down, cols, i) for i in range(4)), n_seq)
        out_q = hop(piece_o)
        up_a = hop(piece_a)
        up_b = hop(piece_b)
        down = [hop(piece_down[0])]
        down_d = tp_swap(piece_down[1])
        lasts = [(down_d, sp_swap(down_d, swap_x), sp_swap(down_d, swap_core))]
        lasts += [(tp_swap(piece_down[2]),), (tp_swap(piece_down[3]),)]

        local_pos = glob_pos - row_start
        pick = (local_pos[:, None] == jnp.arange(local_rows)[None, :]).astype(BF16)
        x_part = project(pick, tokens)
        keep, give = halves(x_part, core)
        keep = keep + sp_swap(give, swap_core)
        keep = keep + sp_swap(keep, swap_x)
        got = sp_swap(keep, swap_core)
        x_glob = jnp.concatenate([jnp.where(core == 0, keep, got), jnp.where(core == 0, got, keep)])

        k_loc = project_rows(tokens, w_key)
        v_loc = project_rows(tokens, w_value)
        kv_l = sp_swap(jnp.concatenate([k_loc[local_rows - window:], v_loc[local_rows - window:]]), to_right)
        kv_r = sp_swap(jnp.concatenate([k_loc[:window], v_loc[:window]]), to_left)
        half = jnp.stack([1 - tp, row_start]).astype(jnp.int32)
        mine = jnp.stack([tp, row_start]).astype(jnp.int32)
        q_loc = project_rows(tokens, w_query)
        qg = project(x_glob, w_query_glob)
        kg = project(x_glob, w_key)
        vg = project(x_glob, w_value)

        state = global_partial(qg, k_loc, v_loc, 256)

        def merge(mine, other):
            top_a, top_b = mine[:, local_dim:local_dim + local_heads], other[:, local_dim:local_dim + local_heads]
            at = local_dim + LANES // 2
            tot_a, tot_b = mine[:, at:at + local_heads], other[:, at:at + local_heads]
            best = jnp.maximum(top_a, top_b)
            fac_a = jnp.exp2(top_a - best)
            fac_b = jnp.exp2(top_b - best)

            def wide(fac):
                return jnp.repeat(fac, LANES, axis=1)

            acc = mine[:, :local_dim] * wide(fac_a) + other[:, :local_dim] * wide(fac_b)
            return acc, best, tot_a * fac_a + tot_b * fac_b

        keep, give = halves(state, core)
        acc, top, tot = merge(keep, sp_swap(give, swap_core))
        fill = jnp.zeros((acc.shape[0], LANES // 2 - local_heads), F32)
        state = jnp.concatenate([acc, top, fill, tot, fill], axis=1)
        keep, give = halves(state, xpos)
        acc, _, tot = merge(keep, sp_swap(give, swap_x))
        g_mine = (acc / jnp.repeat(tot, LANES, axis=1)).astype(BF16)
        g_pair = jnp.concatenate([g_mine, tp_swap(g_mine)], axis=1)
        g_half = jnp.concatenate([g_pair, sp_swap(g_pair, swap_x)])
        g_all = jnp.concatenate([g_half, sp_swap(g_half, swap_core)])
        part = num_glob // n_seq
        order = [core * 2 + xpos, core * 2 + 1 - xpos, (1 - core) * 2 + xpos, (1 - core) * 2 + 1 - xpos]
        gp_order = jnp.concatenate([lax.dynamic_slice_in_dim(glob_pos, i * part, part) for i in order])

        rel = jnp.concatenate([rel_bias * LOG2E, jnp.full((local_heads, window - 1), NEG, F32)], axis=1)[:, None, :]
        gp = glob_pos[None, :]

        def attend(info):
            return window_attention(info, q_loc, k_loc, v_loc, kv_l, kv_r, kg, vg, rel, gp, seq_len, window)

        o_other = tp_swap(attend(half))
        o_own = attend(mine)
        info = jnp.stack([sp, row_start + tp * rows, tp]).astype(jnp.int32)
        hidden = out_proj(info, tokens, o_own, o_other, g_all, gp_order[None, :], w_out, out_q, part_out)
        act = up_proj(info, hidden, w_up, up_a, up_b, part_up)
        return down_proj(hidden, act, w_down, down, lasts, local_rows)

    row_spec = P(("batch", "sp"), None)
    col_spec = P(None, "tp")
    head_spec = P("tp", None)
    in_specs = (row_spec, P("batch"), head_spec, col_spec, col_spec, col_spec, col_spec, head_spec, col_spec, head_spec)
    return jax.shard_map(local_layer, mesh=mesh, in_specs=in_specs, out_specs=row_spec, check_vma=False)
```
